256 devices in a mesh: lat: 4 (over x_lo, core), lon: 4 (over y), lev: 4 (over z_hi, x_hi), unit: 4 (over z_lo).
Axes of the slice: x: 4 (x_hi: 2, x_lo: 2; x = x_hi * 2 + x_lo), y: 4, z: 8 (z_hi: 2, z_lo: 4; z = z_hi * 4 + z_lo), core: 2. Of those that a mesh axis runs over, the one named last changes fastest.
Arguments:
- tracer: float32 [64, 512, 64, 128], P(('unit', 'lat'), 'lon', 'lev'), parts along dimension 0, may hold values from 0.5 to 2
- diffusivity: float32 [64, 512, 64, 128], P(('unit', 'lat'), 'lon', 'lev'), parts along dimension 0, may hold values from 0.03 to 0.15
- source: float32 [64, 512, 64, 128], P(('unit', 'lat'), 'lon', 'lev'), parts along dimension 0, may hold values from -0.2 to 0.2
Outputs:
- standardized: float32 [64, 512, 64, 128], P(('unit', 'lat'), 'lon', 'lev'), parts along dimension 0
- tracer_end: float32 [64, 512, 64, 128], P(('unit', 'lat'), 'lon', 'lev'), parts along dimension 0
The draws below stay inside these ranges and needn't reach their ends.
There are 4 independent parts, one for each index of `unit`. The reference program is written for one: setup_inputs(seed, part) draws one part's arguments, and reference() takes and returns one part's arrays. A program takes and returns all parts, laid end to end along the dimension named above; each array names one. Nothing has to cross between parts.
All inputs are finite; a program needn't handle non-finite values.
Results may differ from the reference program's by a relative error of at most 0.00002.
Values sent between devices are 32-bit elements; how exact they have to be, the bound alone decides.
A program may use at most 128 MiB of HBM per device.

```python
import jax
import jax.numpy as jnp
from jax import lax

GRID_J = 16
GRID_I = 512
GRID_K = 64
LEVELS = 128
STEPS = 4


def steps_of(rng, extent, split, smallest, largest):
    gain = 1.0
    for dim, parts in split:
        steps = jax.random.uniform(jax.random.fold_in(jax.random.fold_in(rng, 6), dim), (parts,), jnp.float32, smallest / len(split), largest / len(split))
        gain = gain * jnp.repeat(jnp.exp(steps), extent[dim] // parts).reshape((-1,) + (1,) * (len(extent) - 1 - dim))
    return gain


def setup_inputs(seed: int = 0, part: int = 0) -> dict:
    streams_of = jax.random.split(jax.random.key(seed), 4)
    part_keys = jax.random.split(jax.random.fold_in(streams_of[3], part), 4)
    return {
        "tracer": jnp.clip(0.5 + 1.5 * jax.random.uniform(part_keys[0], (GRID_J, GRID_I, GRID_K, LEVELS), jnp.float32) ** steps_of(part_keys[0], (GRID_J, GRID_I, GRID_K, LEVELS), ((0, 4), (1, 4), (2, 4)), -0.2, 0.2), 0.5, 2.0),
        "diffusivity": jnp.clip(0.03 + 0.120000007 * jax.random.uniform(part_keys[1], (GRID_J, GRID_I, GRID_K, LEVELS), jnp.float32) ** steps_of(part_keys[1], (GRID_J, GRID_I, GRID_K, LEVELS), ((0, 4), (1, 4), (2, 4)), -0.2, 0.2), 0.03, 0.15),
        "source": jnp.clip(jax.random.uniform(part_keys[2], (GRID_J, GRID_I, GRID_K, LEVELS), jnp.float32, -0.2, 0.2) * steps_of(part_keys[2], (GRID_J, GRID_I, GRID_K, LEVELS), ((0, 4), (1, 4), (2, 4)), -0.4, 0.0), -0.2, 0.2),
    }


def strip_edges(values, dims):
    for dim in dims:
        values = lax.slice_in_dim(values, 1, values.shape[dim] - 1, axis=dim)
    return values

def neighbour(values, dim, start, dims):
    others = [other for other in dims if other != dim]
    values = strip_edges(values, others)
    return lax.slice_in_dim(values, start, start + values.shape[dim] - 2, axis=dim)

def one_step(padded, diffusivity, source):
    middle = strip_edges(padded, (0, 1, 2))
    lower = [neighbour(padded, dim, 0, (0, 1, 2)) for dim in (0, 1, 2)]
    upper = [neighbour(padded, dim, 2, (0, 1, 2)) for dim in (0, 1, 2)]
    spread = lower[0] + upper[0] + lower[1] + upper[1] + lower[2] + upper[2] - 6.0 * middle
    return middle + diffusivity * spread + source

def reference(tracer, diffusivity, source):
    for step in range(STEPS):
        tracer = one_step(jnp.pad(tracer, ((1, 1), (1, 1), (1, 1), (0, 0)), mode='wrap'), diffusivity, source)
    line_mean = lax.optimization_barrier(jnp.mean(tracer, axis=2, keepdims=True))
    centred = tracer - line_mean
    line_variance = lax.optimization_barrier(jnp.mean(centred * centred, axis=2, keepdims=True))
    standardized = centred * lax.rsqrt(line_variance + 0.0001)
    return (standardized, tracer)
```

```python
import functools

import jax
import jax.numpy as jnp
from jax import lax
from jax.experimental import pallas as pl
from jax.experimental.pallas import tpu as pltpu
from jax.sharding import PartitionSpec as P

STEPS = 4
CHUNKS = 8
LAG = 2
MESH = pl.DeviceIdType.MESH
F32 = jnp.float32


def stencil_kernel(
    n_lat, n_lon, n_lev,
    t_hbm, d_hbm, s_hbm,
    end_hbm, stat_hbm,
    te, dv, sv, ksend, khalo, stats, parts, mr,
    load_sem, out_sem, lat_send, lat_recv, lon_send, lon_recv, lev_send, lev_recv,
    rs_send, rs_recv, ag_send, ag_recv,
):
    rows, ni, nk, lanes = t_hbm.shape
    ci = ni // CHUNKS
    lat, lon, lev = lax.axis_index("lat"), lax.axis_index("lon"), lax.axis_index("lev")
    lat_to = ({"lat": lax.rem(lat + 1, n_lat)}, {"lat": lax.rem(lat + n_lat - 1, n_lat)})
    lon_to = ({"lon": lax.rem(lon + 1, n_lon)}, {"lon": lax.rem(lon + n_lon - 1, n_lon)})
    lev_to = [{"lev": lax.rem(lev + d, n_lev)} for d in range(1, n_lev)]

    def inner(c):
        return pl.ds(pl.multiple_of(c * ci, ci), ci)

    def padded(c):
        return pl.ds(1 + c * ci, ci)

    def remote(src, dst, send, recv, to):
        return pltpu.make_async_remote_copy(
            src_ref=src, dst_ref=dst, send_sem=send, recv_sem=recv, device_id=to, device_id_type=MESH
        )

    def lat_copy(t, c, d, first=False):
        row = (rows - 1, 0)[d]
        src = t_hbm.at[row, inner(c)] if first else te.at[t, row + 1, padded(c)]
        return remote(src, te.at[t, (0, rows + 1)[d], padded(c)], lat_send.at[d], lat_recv.at[d, t, c], lat_to[d])

    def lon_copy(t, d, first=False):
        col = (ni - 1, 0)[d]
        src = t_hbm.at[:, col] if first else te.at[t, pl.ds(1, rows), col + 1]
        return remote(src, te.at[t, pl.ds(1, rows), (0, ni + 1)[d]], lon_send.at[d], lon_recv.at[d, t], lon_to[d])

    def lev_copy(t, c, d):
        return remote(
            ksend.at[t, d, :, inner(c)], khalo.at[t, d, :, inner(c)],
            lev_send.at[d], lev_recv.at[d, t, c], lev_to[(0, n_lev - 2)[d]],
        )

    def rs_copy(c, d):
        row = lax.rem(lev + d, n_lev)
        return remote(
            stats.at[row, :, inner(c)], parts.at[d - 1, :, inner(c)],
            rs_send.at[d - 1], rs_recv.at[d - 1, c], lev_to[d - 1],
        )

    def ag_copy(c, d, row):
        return remote(
            mr.at[row, :, inner(c)], mr.at[row, :, inner(c)],
            ag_send.at[d - 1], ag_recv.at[d - 1, c], lev_to[d - 1],
        )

    loads = [
        pltpu.make_async_copy(t_hbm, te.at[0, pl.ds(1, rows), pl.ds(1, ni)], load_sem.at[0]),
        pltpu.make_async_copy(d_hbm, dv, load_sem.at[1]),
        pltpu.make_async_copy(s_hbm, sv, load_sem.at[2]),
    ]
    for load in loads:
        load.start()

    barrier = pltpu.get_barrier_semaphore()
    peers = [*lat_to, *lon_to, *lev_to]
    for peer in peers:
        pl.semaphore_signal(barrier, inc=1, device_id=peer, device_id_type=MESH)
    pl.semaphore_wait(barrier, len(peers))

    def first_lat(c, _):
        for d in (0, 1):
            lat_copy(0, c, d, True).start()
        return 0

    loads[0].wait()
    for d in (0, 1):
        lon_copy(0, d, True).start()

    def first_lev(c, _):
        def row(i, _):
            for j in range(rows):
                ksend[0, 0, j, pl.ds(i, 1), :] = te[0, j + 1, i + 1, pl.ds(nk - 1, 1), :]
                ksend[0, 1, j, pl.ds(i, 1), :] = te[0, j + 1, i + 1, pl.ds(0, 1), :]
            return 0

        lax.fori_loop(c * ci, (c + 1) * ci, row, 0)
        for d in (0, 1):
            lev_copy(0, c, d).start()
            lat_copy(0, c, d, True).start()
        return 0

    lax.fori_loop(0, CHUNKS, first_lev, 0)
    loads[1].wait()
    loads[2].wait()

    k_of = lax.broadcasted_iota(jnp.int32, (nk, lanes), 0)
    bottom, top = k_of == 0, k_of == nk - 1

    def update(t, c, last):
        def column(i, _):
            line = [te[t, j, i + 1] for j in range(rows + 2)]
            for j in range(rows):
                middle = line[j + 1]
                low = khalo[t, 0, j, pl.ds(i, 1), :]
                high = khalo[t, 1, j, pl.ds(i, 1), :]
                below = jnp.where(bottom, jnp.broadcast_to(low, middle.shape), pltpu.roll(middle, 1, 0))
                above = jnp.where(top, jnp.broadcast_to(high, middle.shape), pltpu.roll(middle, nk - 1, 0))
                spread = (
                    line[j] + line[j + 2] + te[t, j + 1, i] + te[t, j + 1, i + 2] + below + above - 6.0 * middle
                )
                new = middle + dv[j, i] * spread + sv[j, i]
                te[t + 1, j + 1, i + 1] = new
                if last:
                    total = jnp.sum(new, axis=0, keepdims=True)
                    off = new - total * (1.0 / nk)
                    stats[j, 0, pl.ds(i, 1), :] = total
                    stats[j, 1, pl.ds(i, 1), :] = jnp.sum(off * off, axis=0, keepdims=True)
                else:
                    ksend[t + 1, 0, j, pl.ds(i, 1), :] = new[nk - 1 :]
                    ksend[t + 1, 1, j, pl.ds(i, 1), :] = new[:1]
            return 0

        lax.fori_loop(c * ci, (c + 1) * ci, column, 0)

    def arrive(t, c):
        for d in (0, 1):
            lat_copy(t, c, d).wait_recv()
            lev_copy(t, c, d).wait_recv()

        @pl.when(c == 0)
        def _():
            lon_copy(t, 0).wait_recv()

        @pl.when(c == CHUNKS - 1)
        def _():
            lon_copy(t, 1).wait_recv()

    def step(t, _):
        def position(p, _):
            c = lax.rem(p + t + 1, CHUNKS)
            arrive(t, c)
            update(t, c, False)
            for d in (0, 1):
                lev_copy(t + 1, c, d).start()
                lat_copy(t + 1, c, d).start()

            @pl.when(c == CHUNKS - 1)
            def _():
                lon_copy(t + 1, 0).start()

            @pl.when(c == 0)
            def _():
                lon_copy(t + 1, 1).start()

            return 0

        return lax.fori_loop(0, CHUNKS, position, 0)

    lax.fori_loop(0, STEPS - 1, step, 0)

    final = STEPS - 1
    count = nk * n_lev

    def end_copy(c):
        return pltpu.make_async_copy(
            te.at[STEPS, pl.ds(1, rows), padded(c)], end_hbm.at[:, inner(c)], out_sem.at[c]
        )

    def chunk_at(p):
        return lax.rem(p + final + 1, CHUNKS)

    def reduce(p):
        c = chunk_at(p)
        for d in range(1, n_lev):
            rs_copy(c, d).wait_recv()
        totals = [stats[lev, 0, inner(c)], *(parts[d, 0, inner(c)] for d in range(n_lev - 1))]
        squares = [stats[lev, 1, inner(c)], *(parts[d, 1, inner(c)] for d in range(n_lev - 1))]
        mean = sum(totals[1:], totals[0]) * (1.0 / count)
        square = sum(squares[1:], squares[0])
        for total in totals:
            gap = total * (1.0 / nk) - mean
            square = square + nk * (gap * gap)
        mr[lev, 0, inner(c)] = mean
        mr[lev, 1, inner(c)] = lax.rsqrt(square * (1.0 / count) + 0.0001)
        for d in range(1, n_lev):
            ag_copy(c, d, lev).start()

    def last_position(p, _):
        c = chunk_at(p)
        arrive(final, c)
        update(final, c, True)
        for d in range(1, n_lev):
            rs_copy(c, d).start()
        end_copy(c).start()

        @pl.when(p >= LAG)
        def _():
            reduce(p - LAG)

        return 0

    lax.fori_loop(0, CHUNKS, last_position, 0)

    def drain(p, _):
        reduce(p)
        return 0

    lax.fori_loop(CHUNKS - LAG, CHUNKS, drain, 0)

    def finish(c, _):
        end_copy(c).wait()
        for d in range(1, n_lev):
            ag_copy(c, d, lax.rem(lev + n_lev - d, n_lev)).wait_recv()
        return 0

    lax.fori_loop(0, CHUNKS, finish, 0)
    out = pltpu.make_async_copy(mr, stat_hbm, load_sem.at[0])
    out.start()

    for d in (0, 1):
        pltpu.make_async_copy(dv, dv, lat_send.at[d]).wait()
        pltpu.make_async_copy(ksend.at[:, d], khalo.at[:, d], lev_send.at[d]).wait()
        whole = te.at[pl.ds(0, STEPS), pl.ds(1, rows), 0]
        pltpu.make_async_copy(whole, whole, lon_send.at[d]).wait()
    for d in range(n_lev - 1):
        pltpu.make_async_copy(parts.at[d], parts.at[d], rs_send.at[d]).wait()
        pltpu.make_async_copy(parts.at[d], parts.at[d], ag_send.at[d]).wait()
    out.wait()


def scale_kernel(t_ref, m_ref, o_ref, e_ref):
    value = t_ref[...]
    e_ref[...] = value
    o_ref[...] = (value - m_ref[:, 0][:, :, None, :]) * m_ref[:, 1][:, :, None, :]


def on_device(sizes, tracer, diffusivity, source):
    rows, ni, nk, lanes = tracer.shape
    n_lat, n_lon, n_lev = sizes
    any_space = pl.BlockSpec(memory_space=pl.ANY)
    dma, vmem = pltpu.SemaphoreType.DMA, pltpu.VMEM
    end, stat = pl.pallas_call(
        functools.partial(stencil_kernel, n_lat, n_lon, n_lev),
        out_shape=(
            jax.ShapeDtypeStruct(tracer.shape, F32),
            jax.ShapeDtypeStruct((rows, 2, ni, lanes), F32),
        ),
        in_specs=[any_space] * 3,
        out_specs=(any_space, any_space),
        scratch_shapes=[
            vmem((STEPS + 1, rows + 2, ni + 2, nk, lanes), F32),
            vmem((rows, ni, nk, lanes), F32),
            vmem((rows, ni, nk, lanes), F32),
            vmem((STEPS, 2, rows, ni, lanes), F32),
            vmem((STEPS, 2, rows, ni, lanes), F32),
            vmem((rows, 2, ni, lanes), F32),
            vmem((n_lev - 1, 2, ni, lanes), F32),
            vmem((rows, 2, ni, lanes), F32),
            dma((3,)), dma((CHUNKS,)),
            dma((2,)), dma((2, STEPS, CHUNKS)),
            dma((2,)), dma((2, STEPS)),
            dma((2,)), dma((2, STEPS, CHUNKS)),
            dma((n_lev - 1,)), dma((n_lev - 1, CHUNKS)),
            dma((n_lev - 1,)), dma((n_lev - 1, CHUNKS)),
        ],
        compiler_params=pltpu.CompilerParams(
            collective_id=0, has_side_effects=True, vmem_limit_bytes=60 * 2**20
        ),
        name="stencil",
    )(tracer, diffusivity, source)
    block = 32
    spec = pl.BlockSpec((1, block, nk, lanes), lambda j, i: (j, i, 0, 0))
    return pl.pallas_call(
        scale_kernel,
        grid=(rows, ni // block),
        out_shape=(jax.ShapeDtypeStruct(tracer.shape, F32), jax.ShapeDtypeStruct(tracer.shape, F32)),
        in_specs=[spec, pl.BlockSpec((1, 2, block, lanes), lambda j, i: (j, 0, i, 0))],
        out_specs=(spec, spec),
        name="scale",
    )(end, stat)


def solution(mesh):
    sizes = (mesh.shape["lat"], mesh.shape["lon"], mesh.shape["lev"])
    spec = P(("unit", "lat"), "lon", "lev", None)
    return jax.shard_map(
        functools.partial(on_device, sizes),
        mesh=mesh,
        in_specs=(spec, spec, spec),
        out_specs=(spec, spec),
        check_vma=False,
    )
```

```python
import functools

import jax
import jax.numpy as jnp
from jax import lax
from jax.experimental import pallas as pl
from jax.experimental.pallas import tpu as pltpu
from jax.sharding import PartitionSpec as P

STEPS = 4
CHUNKS = 8
END_LAG = 4
PAIR_LAG = END_LAG + 2
FAR_LAG = PAIR_LAG + 3
MESH = pl.DeviceIdType.MESH
F32 = jnp.float32


def stencil_kernel(
    n_lat, n_lon, n_lev,
    t_hbm, d_hbm, s_hbm,
    end_ref, stat_ref,
    te, dv, sv, ksend, khalo, stats, parts, paired, far, mr,
    load_sem, lat_send, lat_recv, lon_send, lon_recv, lev_send, lev_recv,
    rs_send, rs_recv, far_send, far_recv, ag_send, ag_recv,
):
    rows, ni, nk, lanes = t_hbm.shape
    ci = ni // CHUNKS
    lat, lon, lev = lax.axis_index("lat"), lax.axis_index("lon"), lax.axis_index("lev")
    lat_to = ({"lat": lax.rem(lat + 1, n_lat)}, {"lat": lax.rem(lat + n_lat - 1, n_lat)})
    lon_to = ({"lon": lax.rem(lon + 1, n_lon)}, {"lon": lax.rem(lon + n_lon - 1, n_lon)})
    lev_to = [{"lev": lax.rem(lev + d, n_lev)} for d in range(1, n_lev)]

    def inner(c):
        return pl.ds(pl.multiple_of(c * ci, ci), ci)

    def padded(c):
        return pl.ds(1 + c * ci, ci)

    def remote(src, dst, send, recv, to):
        return pltpu.make_async_remote_copy(
            src_ref=src, dst_ref=dst, send_sem=send, recv_sem=recv, device_id=to, device_id_type=MESH
        )

    def lat_copy(t, c, d, first=False):
        row = (rows - 1, 0)[d]
        src = t_hbm.at[row, inner(c)] if first else te.at[t, row + 1, padded(c)]
        return remote(src, te.at[t, (0, rows + 1)[d], padded(c)], lat_send.at[d], lat_recv.at[d, t, c], lat_to[d])

    def lon_copy(t, d, first=False):
        col = (ni - 1, 0)[d]
        src = t_hbm.at[:, col] if first else te.at[t, pl.ds(1, rows), col + 1]
        return remote(src, te.at[t, pl.ds(1, rows), (0, ni + 1)[d]], lon_send.at[d], lon_recv.at[d, t], lon_to[d])

    def lev_copy(t, c, d):
        return remote(
            ksend.at[t, d, :, inner(c)], khalo.at[t, d, :, inner(c)],
            lev_send.at[d], lev_recv.at[d, t, c], lev_to[(0, n_lev - 2)[d]],
        )

    half = rows // 2
    side = lax.rem(lev, 2)
    mine, other = pl.ds(half * side, half), pl.ds(half * (1 - side), half)
    pair_to = {"lev": lev + 1 - 2 * side}
    far_to = lev_to[1]

    def rs_copy(c):
        return remote(stats.at[other, :, inner(c)], parts.at[:, :, inner(c)], rs_send.at[0], rs_recv.at[c], pair_to)

    def far_copy(c):
        return remote(paired.at[:, :, inner(c)], far.at[:, :, inner(c)], far_send.at[0], far_recv.at[c], far_to)

    def ag_copy(c, which):
        return remote(mr.at[which, :, inner(c)], mr.at[which, :, inner(c)], ag_send.at[0], ag_recv.at[c], pair_to)

    loads = [
        pltpu.make_async_copy(t_hbm, te.at[0, pl.ds(1, rows), pl.ds(1, ni)], load_sem.at[0]),
        pltpu.make_async_copy(d_hbm, dv, load_sem.at[1]),
        pltpu.make_async_copy(s_hbm, sv, load_sem.at[2]),
    ]
    for load in loads:
        load.start()

    barrier = pltpu.get_barrier_semaphore()
    peers = [*lat_to, *lon_to, *lev_to]
    for peer in peers:
        pl.semaphore_signal(barrier, inc=1, device_id=peer, device_id_type=MESH)
    pl.semaphore_wait(barrier, len(peers))

    loads[0].wait()
    for d in (0, 1):
        lon_copy(0, d, True).start()

    def first_lev(c, _):
        def row(i, _):
            for j in range(rows):
                ksend[0, 0, j, pl.ds(i, 1), :] = te[0, j + 1, i + 1, pl.ds(nk - 1, 1), :]
                ksend[0, 1, j, pl.ds(i, 1), :] = te[0, j + 1, i + 1, pl.ds(0, 1), :]
            return 0

        lax.fori_loop(c * ci, (c + 1) * ci, row, 0)
        for d in (0, 1):
            lev_copy(0, c, d).start()
            lat_copy(0, c, d, True).start()
        return 0

    lax.fori_loop(0, CHUNKS, first_lev, 0)
    loads[1].wait()
    loads[2].wait()

    k_of = lax.broadcasted_iota(jnp.int32, (nk, lanes), 0)
    bottom, top = k_of == 0, k_of == nk - 1

    def update(t, c, last):
        def column(i, _):
            line = [te[t, j, i + 1] for j in range(rows + 2)]
            for j in range(rows):
                middle = line[j + 1]
                low = khalo[t, 0, j, pl.ds(i, 1), :]
                high = khalo[t, 1, j, pl.ds(i, 1), :]
                below = jnp.where(bottom, jnp.broadcast_to(low, middle.shape), pltpu.roll(middle, 1, 0))
                above = jnp.where(top, jnp.broadcast_to(high, middle.shape), pltpu.roll(middle, nk - 1, 0))
                spread = (
                    line[j] + line[j + 2] + te[t, j + 1, i] + te[t, j + 1, i + 2] + below + above - 6.0 * middle
                )
                new = middle + dv[j, i] * spread + sv[j, i]
                if last:
                    end_ref[j, i] = new
                    total = jnp.sum(new, axis=0, keepdims=True)
                    off = new - total * (1.0 / nk)
                    stats[j, 0, pl.ds(i, 1), :] = total
                    stats[j, 1, pl.ds(i, 1), :] = jnp.sum(off * off, axis=0, keepdims=True)
                else:
                    te[t + 1, j + 1, i + 1] = new
                    ksend[t + 1, 0, j, pl.ds(i, 1), :] = new[nk - 1 :]
                    ksend[t + 1, 1, j, pl.ds(i, 1), :] = new[:1]
            return 0

        lax.fori_loop(c * ci, (c + 1) * ci, column, 0)

    def arrive(t, c):
        for d in (0, 1):
            lat_copy(t, c, d).wait_recv()
            lev_copy(t, c, d).wait_recv()

        @pl.when(c == 0)
        def _():
            lon_copy(t, 0).wait_recv()

        @pl.when(c == CHUNKS - 1)
        def _():
            lon_copy(t, 1).wait_recv()

    def position(t, p):
        c = lax.rem(p + t + 1, CHUNKS)
        arrive(t, c)
        update(t, c, False)
        for d in (0, 1):
            lev_copy(t + 1, c, d).start()
            lat_copy(t + 1, c, d).start()

        @pl.when(c == CHUNKS - 1)
        def _():
            lon_copy(t + 1, 0).start()

        @pl.when(c == 0)
        def _():
            lon_copy(t + 1, 1).start()

    def step(g, _):
        position(lax.div(g, CHUNKS), lax.rem(g, CHUNKS))
        return 0

    lax.fori_loop(0, (STEPS - 2) * CHUNKS, step, 0)

    final = STEPS - 1
    count = nk * n_lev

    def chunk_at(p):
        return lax.rem(p + final + 1, CHUNKS)

    def joined(total_a, square_a, total_b, square_b, cells):
        gap = (total_a - total_b) * (1.0 / cells)
        return total_a + total_b, square_a + square_b + (0.5 * cells) * (gap * gap)

    def pair_up(p):
        c = chunk_at(p)
        rs_copy(c).wait_recv()
        for r in range(half):
            row = half * side + r
            total, square = joined(
                stats[row, 0, inner(c)], stats[row, 1, inner(c)], parts[r, 0, inner(c)], parts[r, 1, inner(c)], nk
            )
            paired[r, 0, inner(c)] = total
            paired[r, 1, inner(c)] = square
        far_copy(c).start()

    def reduce(p):
        c = chunk_at(p)
        far_copy(c).wait_recv()
        for r in range(half):
            row = half * side + r
            total, square = joined(
                paired[r, 0, inner(c)], paired[r, 1, inner(c)], far[r, 0, inner(c)], far[r, 1, inner(c)], 2 * nk
            )
            mr[row, 0, inner(c)] = total * (1.0 / count)
            mr[row, 1, inner(c)] = lax.rsqrt(square * (1.0 / count) + 0.0001)
        ag_copy(c, mine).start()

    def last_position(p, _):
        @pl.when(p < CHUNKS)
        def _():
            position(final - 1, p)

        @pl.when((p >= END_LAG) & (p < CHUNKS + END_LAG))
        def _():
            c = chunk_at(p - END_LAG)
            arrive(final, c)
            update(final, c, True)
            rs_copy(c).start()

        @pl.when((p >= PAIR_LAG) & (p < CHUNKS + PAIR_LAG))
        def _():
            pair_up(p - PAIR_LAG)

        @pl.when(p >= FAR_LAG)
        def _():
            reduce(p - FAR_LAG)

        return 0

    lax.fori_loop(0, CHUNKS + FAR_LAG, last_position, 0)

    def finish(c, _):
        ag_copy(c, other).wait_recv()
        return 0

    lax.fori_loop(0, CHUNKS, finish, 0)
    stat_ref[...] = mr[...]

    for d in (0, 1):
        pltpu.make_async_copy(dv, dv, lat_send.at[d]).wait()
        pltpu.make_async_copy(ksend.at[:, d], khalo.at[:, d], lev_send.at[d]).wait()
        whole = te.at[pl.ds(0, STEPS), pl.ds(1, rows), 0]
        pltpu.make_async_copy(whole, whole, lon_send.at[d]).wait()
    for sem in (rs_send, far_send, ag_send):
        pltpu.make_async_copy(parts, far, sem.at[0]).wait()


def scale_kernel(t_ref, m_ref, o_hbm, e_hbm, scaled, sems):
    rows, ni = t_ref.shape[:2]
    ends = pltpu.make_async_copy(t_ref, e_hbm, sems.at[rows])
    ends.start()
    for j in range(rows):

        def column(i, _):
            value = t_ref[j, i]
            mean = jnp.broadcast_to(m_ref[j, 0, pl.ds(i, 1), :], value.shape)
            scale = jnp.broadcast_to(m_ref[j, 1, pl.ds(i, 1), :], value.shape)
            scaled[j, i] = (value - mean) * scale
            return 0

        lax.fori_loop(0, ni, column, 0, unroll=8)
        pltpu.make_async_copy(scaled.at[j], o_hbm.at[j], sems.at[j]).start()
    for j in range(rows):
        pltpu.make_async_copy(scaled.at[j], o_hbm.at[j], sems.at[j]).wait()
    ends.wait()


def on_device(sizes, tracer, diffusivity, source):
    rows, ni, nk, lanes = tracer.shape
    n_lat, n_lon, n_lev = sizes
    any_space = pl.BlockSpec(memory_space=pl.ANY)
    in_vmem = pl.BlockSpec(memory_space=pltpu.VMEM)
    dma, vmem = pltpu.SemaphoreType.DMA, pltpu.VMEM
    end, stat = pl.pallas_call(
        functools.partial(stencil_kernel, n_lat, n_lon, n_lev),
        out_shape=(vmem(tracer.shape, F32), vmem((rows, 2, ni, lanes), F32)),
        in_specs=[any_space] * 3,
        out_specs=(in_vmem, in_vmem),
        scratch_shapes=[
            vmem((STEPS, rows + 2, ni + 2, nk, lanes), F32),
            vmem((rows, ni, nk, lanes), F32),
            vmem((rows, ni, nk, lanes), F32),
            vmem((STEPS, 2, rows, ni, lanes), F32),
            vmem((STEPS, 2, rows, ni, lanes), F32),
            vmem((rows, 2, ni, lanes), F32),
            vmem((rows // 2, 2, ni, lanes), F32),
            vmem((rows // 2, 2, ni, lanes), F32),
            vmem((rows // 2, 2, ni, lanes), F32),
            vmem((rows, 2, ni, lanes), F32),
            dma((3,)),
            dma((2,)), dma((2, STEPS, CHUNKS)),
            dma((2,)), dma((2, STEPS)),
            dma((2,)), dma((2, STEPS, CHUNKS)),
            dma((1,)), dma((CHUNKS,)),
            dma((1,)), dma((CHUNKS,)),
            dma((1,)), dma((CHUNKS,)),
        ],
        compiler_params=pltpu.CompilerParams(
            collective_id=0, has_side_effects=True, vmem_limit_bytes=48 * 2**20
        ),
        name="stencil",
    )(tracer, diffusivity, source)
    whole = jax.ShapeDtypeStruct(tracer.shape, F32)
    return pl.pallas_call(
        scale_kernel,
        out_shape=(whole, whole),
        in_specs=[in_vmem, in_vmem],
        out_specs=(any_space, any_space),
        scratch_shapes=[vmem(tracer.shape, F32), dma((rows + 1,))],
        compiler_params=pltpu.CompilerParams(vmem_limit_bytes=6 * 2**20),
        name="scale",
    )(end, stat)


def solution(mesh):
    sizes = (mesh.shape["lat"], mesh.shape["lon"], mesh.shape["lev"])
    spec = P(("unit", "lat"), "lon", "lev", None)
    return jax.shard_map(
        functools.partial(on_device, sizes),
        mesh=mesh,
        in_specs=(spec, spec, spec),
        out_specs=(spec, spec),
        check_vma=False,
    )
```

```python
import functools

import jax
import jax.numpy as jnp
from jax import lax
from jax.experimental import pallas as pl
from jax.experimental.pallas import tpu as pltpu
from jax.sharding import PartitionSpec as P

STEPS = 4
CHUNKS = 8
EAGER = 2
AHEAD = 2
END_AHEAD = 2
END_LAG = 5
PAIR_LAG = END_LAG + 2
FAR_LAG = PAIR_LAG + 3
MESH = pl.DeviceIdType.MESH
F32 = jnp.float32


def stencil_kernel(
    n_lat, n_lon, n_lev,
    t_hbm, d_hbm, s_hbm,
    end_ref, stat_ref,
    te, dv, sv, ksend, khalo, kon, stats, parts, paired, far, mr,
    load_sem, lat_send, lat_recv, lon_send, lon_recv, lev_send, lev_recv, on_send, on_recv,
    rs_send, rs_recv, far_send, far_recv, ag_send, ag_recv,
):
    rows, ni, nk, lanes = t_hbm.shape
    ci = ni // CHUNKS
    lat, lon, lev = lax.axis_index("lat"), lax.axis_index("lon"), lax.axis_index("lev")
    lat_to = ({"lat": lax.rem(lat + 1, n_lat)}, {"lat": lax.rem(lat + n_lat - 1, n_lat)})
    lon_to = ({"lon": lax.rem(lon + 1, n_lon)}, {"lon": lax.rem(lon + n_lon - 1, n_lon)})
    lev_to = [{"lev": lax.rem(lev + d, n_lev)} for d in range(1, n_lev)]

    def inner(c):
        return pl.ds(pl.multiple_of(c * ci, ci), ci)

    def padded(c):
        return pl.ds(1 + c * ci, ci)

    def remote(src, dst, send, recv, to):
        return pltpu.make_async_remote_copy(
            src_ref=src, dst_ref=dst, send_sem=send, recv_sem=recv, device_id=to, device_id_type=MESH
        )

    def lat_copy(t, c, d, first=False):
        row = (rows - 1, 0)[d]
        src = t_hbm.at[row, inner(c)] if first else te.at[t, row + 1, padded(c)]
        return remote(src, te.at[t, (0, rows + 1)[d], padded(c)], lat_send.at[d], lat_recv.at[d, t, c], lat_to[d])

    def lon_copy(t, d, first=False):
        col = (ni - 1, 0)[d]
        src = t_hbm.at[:, col] if first else te.at[t, pl.ds(1, rows), col + 1]
        return remote(src, te.at[t, pl.ds(1, rows), (0, ni + 1)[d]], lon_send.at[d], lon_recv.at[d, t], lon_to[d])

    odd = lax.rem(lat, 2)
    facing = lax.rem(lat + n_lat + 2 * odd - 1, n_lat)
    sent_rows, my_row, its_row = pl.ds(1 - odd, rows - 1), (rows - 1) * odd, (rows - 1) * (1 - odd)
    on_to = [{"lat": facing, "lev": lax.rem(lev + 1, n_lev)}, {"lat": facing, "lev": lax.rem(lev + n_lev - 1, n_lev)}]

    def lev_copy(t, c, d):
        return remote(
            ksend.at[t, d, sent_rows, inner(c)], khalo.at[t, d, sent_rows, inner(c)],
            lev_send.at[d], lev_recv.at[d, t, c], lev_to[(0, n_lev - 2)[d]],
        )

    def on_copy(t, c, d, row):
        return remote(
            kon.at[t, d, inner(c)], khalo.at[t, d, row, inner(c)], on_send.at[d], on_recv.at[d, t, c], on_to[d]
        )

    def lat_wait(t, c, d):
        halo = te.at[t, (rows + 1) * d, padded(c)]
        remote(halo, halo, lat_send.at[d], lat_recv.at[d, t, c], lat_to[0]).wait_recv()

    def hand_on(t, p):
        c = lax.rem(p + t + 1, CHUNKS)
        lat_wait(t, c, odd)
        halo = (rows + 1) * odd

        def row(i, _):
            kon[t, 0, pl.ds(i, 1), :] = te[t, halo, i + 1, pl.ds(nk - 1, 1), :]
            kon[t, 1, pl.ds(i, 1), :] = te[t, halo, i + 1, pl.ds(0, 1), :]
            return 0

        lax.fori_loop(c * ci, (c + 1) * ci, row, 0)
        for d in (0, 1):
            on_copy(t, c, d, its_row).start()

    half = rows // 2
    side = lax.rem(lev, 2)
    mine, other = pl.ds(half * side, half), pl.ds(half * (1 - side), half)
    pair_to = {"lev": lev + 1 - 2 * side}
    far_to = lev_to[1]

    def rs_copy(c):
        return remote(stats.at[other, :, inner(c)], parts.at[:, :, inner(c)], rs_send.at[0], rs_recv.at[c], pair_to)

    def far_copy(c):
        return remote(paired.at[:, :, inner(c)], far.at[:, :, inner(c)], far_send.at[0], far_recv.at[c], far_to)

    def ag_copy(c, which):
        return remote(mr.at[which, :, inner(c)], mr.at[which, :, inner(c)], ag_send.at[0], ag_recv.at[c], pair_to)

    loads = [
        pltpu.make_async_copy(t_hbm, te.at[0, pl.ds(1, rows), pl.ds(1, ni)], load_sem.at[0]),
        pltpu.make_async_copy(d_hbm, dv, load_sem.at[1]),
        pltpu.make_async_copy(s_hbm, sv, load_sem.at[2]),
    ]
    loads[0].start()

    barrier = pltpu.get_barrier_semaphore()
    peers = [*lat_to, *lon_to, *lev_to, *on_to]
    for peer in peers:
        pl.semaphore_signal(barrier, inc=1, device_id=peer, device_id_type=MESH)
    pl.semaphore_wait(barrier, len(peers))

    def first_lat(c, _):
        for d in (0, 1):
            lat_copy(0, c, d, True).start()
        return 0

    lax.fori_loop(0, EAGER, first_lat, 0)
    for load in loads[1:]:
        load.start()
    for d in (0, 1):
        lon_copy(0, d, True).start()
    loads[0].wait()

    def first_lev(c, _):
        def row(i, _):
            for j in range(rows):
                ksend[0, 0, j, pl.ds(i, 1), :] = te[0, j + 1, i + 1, pl.ds(nk - 1, 1), :]
                ksend[0, 1, j, pl.ds(i, 1), :] = te[0, j + 1, i + 1, pl.ds(0, 1), :]
            return 0

        lax.fori_loop(c * ci, (c + 1) * ci, row, 0)
        for d in (0, 1):
            lev_copy(0, c, d).start()

        @pl.when(c + EAGER < CHUNKS)
        def _():
            first_lat(c + EAGER, 0)

        return 0

    lax.fori_loop(0, CHUNKS, first_lev, 0)
    loads[1].wait()
    loads[2].wait()

    k_of = lax.broadcasted_iota(jnp.int32, (nk, lanes), 0)
    bottom, top = k_of == 0, k_of == nk - 1

    def update(t, c, last):
        def column(i, _):
            line = [te[t, j, i + 1] for j in range(rows + 2)]
            for j in range(rows):
                middle = line[j + 1]
                low = khalo[t, 0, j, pl.ds(i, 1), :]
                high = khalo[t, 1, j, pl.ds(i, 1), :]
                below = jnp.where(bottom, jnp.broadcast_to(low, middle.shape), pltpu.roll(middle, 1, 0))
                above = jnp.where(top, jnp.broadcast_to(high, middle.shape), pltpu.roll(middle, nk - 1, 0))
                spread = (
                    line[j] + line[j + 2] + te[t, j + 1, i] + te[t, j + 1, i + 2] + below + above - 6.0 * middle
                )
                new = middle + dv[j, i] * spread + sv[j, i]
                if last:
                    end_ref[j, i] = new
                    total = jnp.sum(new, axis=0, keepdims=True)
                    off = new - total * (1.0 / nk)
                    stats[j, 0, pl.ds(i, 1), :] = total
                    stats[j, 1, pl.ds(i, 1), :] = jnp.sum(off * off, axis=0, keepdims=True)
                else:
                    te[t + 1, j + 1, i + 1] = new
                    ksend[t + 1, 0, j, pl.ds(i, 1), :] = new[nk - 1 :]
                    ksend[t + 1, 1, j, pl.ds(i, 1), :] = new[:1]
            return 0

        lax.fori_loop(c * ci, (c + 1) * ci, column, 0)

    def arrive(t, c):
        lat_wait(t, c, 1 - odd)
        for d in (0, 1):
            lev_copy(t, c, d).wait_recv()
            on_copy(t, c, d, my_row).wait_recv()

        @pl.when(c == 0)
        def _():
            lon_copy(t, 0).wait_recv()

        @pl.when(c == CHUNKS - 1)
        def _():
            lon_copy(t, 1).wait_recv()

    def position(t, p):
        c = lax.rem(p + t + 1, CHUNKS)
        arrive(t, c)
        update(t, c, False)
        for d in (0, 1):
            lev_copy(t + 1, c, d).start()
            lat_copy(t + 1, c, d).start()

        @pl.when(c == CHUNKS - 1)
        def _():
            lon_copy(t + 1, 0).start()

        @pl.when(c == 0)
        def _():
            lon_copy(t + 1, 1).start()

    def step(g, _):
        hand_on(lax.div(g + AHEAD, CHUNKS), lax.rem(g + AHEAD, CHUNKS))
        position(lax.div(g, CHUNKS), lax.rem(g, CHUNKS))
        return 0

    def first_on(p, _):
        hand_on(0, p)
        return 0

    lax.fori_loop(0, AHEAD, first_on, 0)
    lax.fori_loop(0, (STEPS - 2) * CHUNKS, step, 0)

    final = STEPS - 1
    count = nk * n_lev

    def chunk_at(p):
        return lax.rem(p + final + 1, CHUNKS)

    def joined(total_a, square_a, total_b, square_b, cells):
        gap = (total_a - total_b) * (1.0 / cells)
        return total_a + total_b, square_a + square_b + (0.5 * cells) * (gap * gap)

    def pair_up(p):
        c = chunk_at(p)
        rs_copy(c).wait_recv()
        for r in range(half):
            row = half * side + r
            total, square = joined(
                stats[row, 0, inner(c)], stats[row, 1, inner(c)], parts[r, 0, inner(c)], parts[r, 1, inner(c)], nk
            )
            paired[r, 0, inner(c)] = total
            paired[r, 1, inner(c)] = square
        far_copy(c).start()

    def reduce(p):
        c = chunk_at(p)
        far_copy(c).wait_recv()
        for r in range(half):
            row = half * side + r
            total, square = joined(
                paired[r, 0, inner(c)], paired[r, 1, inner(c)], far[r, 0, inner(c)], far[r, 1, inner(c)], 2 * nk
            )
            mr[row, 0, inner(c)] = total * (1.0 / count)
            mr[row, 1, inner(c)] = lax.rsqrt(square * (1.0 / count) + 0.0001)
        ag_copy(c, mine).start()

    def last_position(p, _):
        @pl.when(p < CHUNKS - AHEAD)
        def _():
            hand_on(final - 1, p + AHEAD)

        @pl.when(p < CHUNKS)
        def _():
            position(final - 1, p)

        @pl.when((p >= END_LAG - END_AHEAD) & (p < CHUNKS + END_LAG - END_AHEAD))
        def _():
            hand_on(final, p - END_LAG + END_AHEAD)

        @pl.when((p >= END_LAG) & (p < CHUNKS + END_LAG))
        def _():
            c = chunk_at(p - END_LAG)
            arrive(final, c)
            update(final, c, True)
            rs_copy(c).start()

        @pl.when((p >= PAIR_LAG) & (p < CHUNKS + PAIR_LAG))
        def _():
            pair_up(p - PAIR_LAG)

        @pl.when(p >= FAR_LAG)
        def _():
            reduce(p - FAR_LAG)

        return 0

    lax.fori_loop(0, CHUNKS + FAR_LAG, last_position, 0)

    def finish(c, _):
        ag_copy(c, other).wait_recv()
        return 0

    lax.fori_loop(0, CHUNKS, finish, 0)
    stat_ref[...] = mr[...]

    for d in (0, 1):
        pltpu.make_async_copy(dv, dv, lat_send.at[d]).wait()
        edges = ksend.at[:, d, pl.ds(0, rows - 1)]
        pltpu.make_async_copy(edges, edges, lev_send.at[d]).wait()
        pltpu.make_async_copy(kon.at[:, d], kon.at[:, d], on_send.at[d]).wait()
        whole = te.at[pl.ds(0, STEPS), pl.ds(1, rows), 0]
        pltpu.make_async_copy(whole, whole, lon_send.at[d]).wait()
    for sem in (rs_send, far_send, ag_send):
        pltpu.make_async_copy(parts, far, sem.at[0]).wait()


def scale_kernel(t_ref, m_ref, o_hbm, e_hbm, scaled, sems):
    rows, ni = t_ref.shape[:2]
    ends = pltpu.make_async_copy(t_ref, e_hbm, sems.at[rows])
    ends.start()
    for j in range(rows):

        def column(i, _):
            value = t_ref[j, i]
            mean = jnp.broadcast_to(m_ref[j, 0, pl.ds(i, 1), :], value.shape)
            scale = jnp.broadcast_to(m_ref[j, 1, pl.ds(i, 1), :], value.shape)
            scaled[j, i] = (value - mean) * scale
            return 0

        lax.fori_loop(0, ni, column, 0, unroll=8)
        pltpu.make_async_copy(scaled.at[j], o_hbm.at[j], sems.at[j]).start()
    for j in range(rows):
        pltpu.make_async_copy(scaled.at[j], o_hbm.at[j], sems.at[j]).wait()
    ends.wait()


def on_device(sizes, tracer, diffusivity, source):
    rows, ni, nk, lanes = tracer.shape
    n_lat, n_lon, n_lev = sizes
    any_space = pl.BlockSpec(memory_space=pl.ANY)
    in_vmem = pl.BlockSpec(memory_space=pltpu.VMEM)
    dma, vmem = pltpu.SemaphoreType.DMA, pltpu.VMEM
    end, stat = pl.pallas_call(
        functools.partial(stencil_kernel, n_lat, n_lon, n_lev),
        out_shape=(vmem(tracer.shape, F32), vmem((rows, 2, ni, lanes), F32)),
        in_specs=[any_space] * 3,
        out_specs=(in_vmem, in_vmem),
        scratch_shapes=[
            vmem((STEPS, rows + 2, ni + 2, nk, lanes), F32),
            vmem((rows, ni, nk, lanes), F32),
            vmem((rows, ni, nk, lanes), F32),
            vmem((STEPS, 2, rows, ni, lanes), F32),
            vmem((STEPS, 2, rows, ni, lanes), F32),
            vmem((STEPS, 2, ni, lanes), F32),
            vmem((rows, 2, ni, lanes), F32),
            vmem((rows // 2, 2, ni, lanes), F32),
            vmem((rows // 2, 2, ni, lanes), F32),
            vmem((rows // 2, 2, ni, lanes), F32),
            vmem((rows, 2, ni, lanes), F32),
            dma((3,)),
            dma((2,)), dma((2, STEPS, CHUNKS)),
            dma((2,)), dma((2, STEPS)),
            dma((2,)), dma((2, STEPS, CHUNKS)),
            dma((2,)), dma((2, STEPS, CHUNKS)),
            dma((1,)), dma((CHUNKS,)),
            dma((1,)), dma((CHUNKS,)),
            dma((1,)), dma((CHUNKS,)),
        ],
        compiler_params=pltpu.CompilerParams(
            collective_id=0, has_side_effects=True, vmem_limit_bytes=48 * 2**20
        ),
        name="stencil",
    )(tracer, diffusivity, source)
    whole = jax.ShapeDtypeStruct(tracer.shape, F32)
    return pl.pallas_call(
        scale_kernel,
        out_shape=(whole, whole),
        in_specs=[in_vmem, in_vmem],
        out_specs=(any_space, any_space),
        scratch_shapes=[vmem(tracer.shape, F32), dma((rows + 1,))],
        compiler_params=pltpu.CompilerParams(vmem_limit_bytes=6 * 2**20),
        name="scale",
    )(end, stat)


def solution(mesh):
    sizes = (mesh.shape["lat"], mesh.shape["lon"], mesh.shape["lev"])
    spec = P(("unit", "lat"), "lon", "lev", None)
    return jax.shard_map(
        functools.partial(on_device, sizes),
        mesh=mesh,
        in_specs=(spec, spec, spec),
        out_specs=(spec, spec),
        check_vma=False,
    )
```

```python
import functools

import jax
import jax.numpy as jnp
from jax import lax
from jax.experimental import pallas as pl
from jax.experimental.pallas import tpu as pltpu
from jax.sharding import PartitionSpec as P

STEPS = 4
CHUNKS = 8
EAGER = 2
AHEAD = 2
END_AHEAD = 2
END_LAG = 5
PAIR_LAG = END_LAG + 3
FAR_LAG = PAIR_LAG + 2
MESH = pl.DeviceIdType.MESH
F32 = jnp.float32


def stencil_kernel(
    n_lat, n_lon, n_lev,
    t_hbm, d_hbm, s_hbm,
    end_ref, stat_ref,
    te, dv, sv, ksend, khalo, kon, stats, parts, paired, far,
    load_sem, lat_send, lat_recv, lon_send, lon_recv, lev_send, lev_recv, on_send, on_recv,
    pair_send, pair_recv, far_send, far_recv,
):
    rows, ni, nk, lanes = t_hbm.shape
    ci = ni // CHUNKS
    lat, lon, lev = lax.axis_index("lat"), lax.axis_index("lon"), lax.axis_index("lev")
    lat_to = ({"lat": lax.rem(lat + 1, n_lat)}, {"lat": lax.rem(lat + n_lat - 1, n_lat)})
    lon_to = ({"lon": lax.rem(lon + 1, n_lon)}, {"lon": lax.rem(lon + n_lon - 1, n_lon)})
    lev_to = [{"lev": lax.rem(lev + d, n_lev)} for d in range(1, n_lev)]

    def inner(c):
        return pl.ds(pl.multiple_of(c * ci, ci), ci)

    def padded(c):
        return pl.ds(1 + c * ci, ci)

    def remote(src, dst, send, recv, to):
        return pltpu.make_async_remote_copy(
            src_ref=src, dst_ref=dst, send_sem=send, recv_sem=recv, device_id=to, device_id_type=MESH
        )

    def lat_copy(t, c, d, first=False):
        row = (rows - 1, 0)[d]
        src = t_hbm.at[row, inner(c)] if first else te.at[t, row + 1, padded(c)]
        return remote(src, te.at[t, (0, rows + 1)[d], padded(c)], lat_send.at[d], lat_recv.at[d, t, c], lat_to[d])

    def lon_copy(t, d, first=False):
        col = (ni - 1, 0)[d]
        src = t_hbm.at[:, col] if first else te.at[t, pl.ds(1, rows), col + 1]
        return remote(src, te.at[t, pl.ds(1, rows), (0, ni + 1)[d]], lon_send.at[d], lon_recv.at[d, t], lon_to[d])

    odd = lax.rem(lat, 2)
    facing = lax.rem(lat + n_lat + 2 * odd - 1, n_lat)
    sent_rows, my_row, its_row = pl.ds(1 - odd, rows - 1), (rows - 1) * odd, (rows - 1) * (1 - odd)
    on_to = [{"lat": facing, "lev": lax.rem(lev + 1, n_lev)}, {"lat": facing, "lev": lax.rem(lev + n_lev - 1, n_lev)}]

    def lev_copy(t, c, d):
        return remote(
            ksend.at[t, d, sent_rows, inner(c)], khalo.at[t, d, sent_rows, inner(c)],
            lev_send.at[d], lev_recv.at[d, t, c], lev_to[(0, n_lev - 2)[d]],
        )

    def on_copy(t, c, d, row):
        return remote(
            kon.at[t, d, inner(c)], khalo.at[t, d, row, inner(c)], on_send.at[d], on_recv.at[d, t, c], on_to[d]
        )

    def lat_wait(t, c, d):
        halo = te.at[t, (rows + 1) * d, padded(c)]
        remote(halo, halo, lat_send.at[d], lat_recv.at[d, t, c], lat_to[0]).wait_recv()

    def hand_on(t, p):
        c = lax.rem(p + t + 1, CHUNKS)
        lat_wait(t, c, odd)
        halo = (rows + 1) * odd

        def row(i, _):
            kon[t, 0, pl.ds(i, 1), :] = te[t, halo, i + 1, pl.ds(nk - 1, 1), :]
            kon[t, 1, pl.ds(i, 1), :] = te[t, halo, i + 1, pl.ds(0, 1), :]
            return 0

        lax.fori_loop(c * ci, (c + 1) * ci, row, 0)
        for d in (0, 1):
            on_copy(t, c, d, its_row).start()

    pair_to, far_to = {"lev": lev + 1 - 2 * lax.rem(lev, 2)}, lev_to[1]

    def first_copy(c):
        return remote(stats.at[:, :, inner(c)], parts.at[:, :, inner(c)], pair_send.at[0], pair_recv.at[c], far_to)

    def second_copy(c):
        return remote(paired.at[:, :, inner(c)], far.at[:, :, inner(c)], far_send.at[0], far_recv.at[c], pair_to)

    loads = [
        pltpu.make_async_copy(t_hbm, te.at[0, pl.ds(1, rows), pl.ds(1, ni)], load_sem.at[0]),
        pltpu.make_async_copy(d_hbm, dv, load_sem.at[1]),
        pltpu.make_async_copy(s_hbm, sv, load_sem.at[2]),
    ]
    loads[0].start()

    barrier = pltpu.get_barrier_semaphore()
    peers = [*lat_to, *lon_to, *lev_to, *on_to]
    for peer in peers:
        pl.semaphore_signal(barrier, inc=1, device_id=peer, device_id_type=MESH)
    pl.semaphore_wait(barrier, len(peers))

    def first_lat(c, _):
        for d in (0, 1):
            lat_copy(0, c, d, True).start()
        return 0

    lax.fori_loop(0, EAGER, first_lat, 0)
    for load in loads[1:]:
        load.start()
    for d in (0, 1):
        lon_copy(0, d, True).start()
    loads[0].wait()

    def first_lev(c, _):
        def row(i, _):
            for j in range(rows):
                ksend[0, 0, j, pl.ds(i, 1), :] = te[0, j + 1, i + 1, pl.ds(nk - 1, 1), :]
                ksend[0, 1, j, pl.ds(i, 1), :] = te[0, j + 1, i + 1, pl.ds(0, 1), :]
            return 0

        lax.fori_loop(c * ci, (c + 1) * ci, row, 0)
        for d in (0, 1):
            lev_copy(0, c, d).start()

        @pl.when(c + EAGER < CHUNKS)
        def _():
            first_lat(c + EAGER, 0)

        return 0

    lax.fori_loop(0, CHUNKS, first_lev, 0)
    loads[1].wait()
    loads[2].wait()

    k_of = lax.broadcasted_iota(jnp.int32, (nk, lanes), 0)
    bottom, top = k_of == 0, k_of == nk - 1

    def update(t, c, last):
        def column(i, _):
            line = [te[t, j, i + 1] for j in range(rows + 2)]
            for j in range(rows):
                middle = line[j + 1]
                low = khalo[t, 0, j, pl.ds(i, 1), :]
                high = khalo[t, 1, j, pl.ds(i, 1), :]
                below = jnp.where(bottom, jnp.broadcast_to(low, middle.shape), pltpu.roll(middle, 1, 0))
                above = jnp.where(top, jnp.broadcast_to(high, middle.shape), pltpu.roll(middle, nk - 1, 0))
                spread = (
                    line[j] + line[j + 2] + te[t, j + 1, i] + te[t, j + 1, i + 2] + below + above - 6.0 * middle
                )
                new = middle + dv[j, i] * spread + sv[j, i]
                if last:
                    end_ref[j, i] = new
                    total = jnp.sum(new, axis=0, keepdims=True)
                    off = new - total * (1.0 / nk)
                    stats[j, 0, pl.ds(i, 1), :] = total
                    stats[j, 1, pl.ds(i, 1), :] = jnp.sum(off * off, axis=0, keepdims=True)
                else:
                    te[t + 1, j + 1, i + 1] = new
                    ksend[t + 1, 0, j, pl.ds(i, 1), :] = new[nk - 1 :]
                    ksend[t + 1, 1, j, pl.ds(i, 1), :] = new[:1]
            return 0

        lax.fori_loop(c * ci, (c + 1) * ci, column, 0)

    def arrive(t, c):
        lat_wait(t, c, 1 - odd)
        for d in (0, 1):
            lev_copy(t, c, d).wait_recv()
            on_copy(t, c, d, my_row).wait_recv()

        @pl.when(c == 0)
        def _():
            lon_copy(t, 0).wait_recv()

        @pl.when(c == CHUNKS - 1)
        def _():
            lon_copy(t, 1).wait_recv()

    def position(t, p):
        c = lax.rem(p + t + 1, CHUNKS)
        arrive(t, c)
        update(t, c, False)
        for d in (0, 1):
            lev_copy(t + 1, c, d).start()
            lat_copy(t + 1, c, d).start()

        @pl.when(c == CHUNKS - 1)
        def _():
            lon_copy(t + 1, 0).start()

        @pl.when(c == 0)
        def _():
            lon_copy(t + 1, 1).start()

    def step(g, _):
        hand_on(lax.div(g + AHEAD, CHUNKS), lax.rem(g + AHEAD, CHUNKS))
        position(lax.div(g, CHUNKS), lax.rem(g, CHUNKS))
        return 0

    def first_on(p, _):
        hand_on(0, p)
        return 0

    lax.fori_loop(0, AHEAD, first_on, 0)
    lax.fori_loop(0, (STEPS - 2) * CHUNKS, step, 0)

    final = STEPS - 1
    count = nk * n_lev

    def chunk_at(p):
        return lax.rem(p + final + 1, CHUNKS)

    def joined(total_a, square_a, total_b, square_b, cells):
        gap = (total_a - total_b) * (1.0 / cells)
        return total_a + total_b, square_a + square_b + (0.5 * cells) * (gap * gap)

    def pair_up(p):
        c = chunk_at(p)
        first_copy(c).wait_recv()
        for r in range(rows):
            total, square = joined(
                stats[r, 0, inner(c)], stats[r, 1, inner(c)], parts[r, 0, inner(c)], parts[r, 1, inner(c)], nk
            )
            paired[r, 0, inner(c)] = total
            paired[r, 1, inner(c)] = square
        second_copy(c).start()

    def reduce(p):
        c = chunk_at(p)
        second_copy(c).wait_recv()
        for r in range(rows):
            total, square = joined(
                paired[r, 0, inner(c)], paired[r, 1, inner(c)], far[r, 0, inner(c)], far[r, 1, inner(c)], 2 * nk
            )
            stat_ref[r, 0, inner(c)] = total * (1.0 / count)
            stat_ref[r, 1, inner(c)] = lax.rsqrt(square * (1.0 / count) + 0.0001)

    def last_position(p, _):
        @pl.when(p < CHUNKS - AHEAD)
        def _():
            hand_on(final - 1, p + AHEAD)

        @pl.when(p < CHUNKS)
        def _():
            position(final - 1, p)

        @pl.when((p >= END_LAG - END_AHEAD) & (p < CHUNKS + END_LAG - END_AHEAD))
        def _():
            hand_on(final, p - END_LAG + END_AHEAD)

        @pl.when((p >= END_LAG) & (p < CHUNKS + END_LAG))
        def _():
            c = chunk_at(p - END_LAG)
            arrive(final, c)
            update(final, c, True)
            first_copy(c).start()

        @pl.when((p >= PAIR_LAG) & (p < CHUNKS + PAIR_LAG))
        def _():
            pair_up(p - PAIR_LAG)

        @pl.when(p >= FAR_LAG)
        def _():
            reduce(p - FAR_LAG)

        return 0

    lax.fori_loop(0, CHUNKS + FAR_LAG, last_position, 0)

    for d in (0, 1):
        pltpu.make_async_copy(dv, dv, lat_send.at[d]).wait()
        edges = ksend.at[:, d, pl.ds(0, rows - 1)]
        pltpu.make_async_copy(edges, edges, lev_send.at[d]).wait()
        pltpu.make_async_copy(kon.at[:, d], kon.at[:, d], on_send.at[d]).wait()
        whole = te.at[pl.ds(0, STEPS), pl.ds(1, rows), 0]
        pltpu.make_async_copy(whole, whole, lon_send.at[d]).wait()
    for sem in (pair_send, far_send):
        pltpu.make_async_copy(parts, far, sem.at[0]).wait()


def scale_kernel(t_ref, m_ref, o_hbm, e_hbm, scaled, sems):
    rows, ni = t_ref.shape[:2]
    ends = pltpu.make_async_copy(t_ref, e_hbm, sems.at[rows])
    ends.start()
    for j in range(rows):

        def column(i, _):
            value = t_ref[j, i]
            mean = jnp.broadcast_to(m_ref[j, 0, pl.ds(i, 1), :], value.shape)
            scale = jnp.broadcast_to(m_ref[j, 1, pl.ds(i, 1), :], value.shape)
            scaled[j, i] = (value - mean) * scale
            return 0

        lax.fori_loop(0, ni, column, 0, unroll=8)
        pltpu.make_async_copy(scaled.at[j], o_hbm.at[j], sems.at[j]).start()
    for j in range(rows):
        pltpu.make_async_copy(scaled.at[j], o_hbm.at[j], sems.at[j]).wait()
    ends.wait()


def on_device(sizes, tracer, diffusivity, source):
    rows, ni, nk, lanes = tracer.shape
    n_lat, n_lon, n_lev = sizes
    any_space = pl.BlockSpec(memory_space=pl.ANY)
    in_vmem = pl.BlockSpec(memory_space=pltpu.VMEM)
    dma, vmem = pltpu.SemaphoreType.DMA, pltpu.VMEM
    end, stat = pl.pallas_call(
        functools.partial(stencil_kernel, n_lat, n_lon, n_lev),
        out_shape=(vmem(tracer.shape, F32), vmem((rows, 2, ni, lanes), F32)),
        in_specs=[any_space] * 3,
        out_specs=(in_vmem, in_vmem),
        scratch_shapes=[
            vmem((STEPS, rows + 2, ni + 2, nk, lanes), F32),
            vmem((rows, ni, nk, lanes), F32),
            vmem((rows, ni, nk, lanes), F32),
            vmem((STEPS, 2, rows, ni, lanes), F32),
            vmem((STEPS, 2, rows, ni, lanes), F32),
            vmem((STEPS, 2, ni, lanes), F32),
            vmem((rows, 2, ni, lanes), F32),
            vmem((rows, 2, ni, lanes), F32),
            vmem((rows, 2, ni, lanes), F32),
            vmem((rows, 2, ni, lanes), F32),
            dma((3,)),
            dma((2,)), dma((2, STEPS, CHUNKS)),
            dma((2,)), dma((2, STEPS)),
            dma((2,)), dma((2, STEPS, CHUNKS)),
            dma((2,)), dma((2, STEPS, CHUNKS)),
            dma((1,)), dma((CHUNKS,)),
            dma((1,)), dma((CHUNKS,)),
        ],
        compiler_params=pltpu.CompilerParams(
            collective_id=0, has_side_effects=True, vmem_limit_bytes=48 * 2**20
        ),
        name="stencil",
    )(tracer, diffusivity, source)
    whole = jax.ShapeDtypeStruct(tracer.shape, F32)
    return pl.pallas_call(
        scale_kernel,
        out_shape=(whole, whole),
        in_specs=[in_vmem, in_vmem],
        out_specs=(any_space, any_space),
        scratch_shapes=[vmem(tracer.shape, F32), dma((rows + 1,))],
        compiler_params=pltpu.CompilerParams(vmem_limit_bytes=6 * 2**20),
        name="scale",
    )(end, stat)


def solution(mesh):
    sizes = (mesh.shape["lat"], mesh.shape["lon"], mesh.shape["lev"])
    spec = P(("unit", "lat"), "lon", "lev", None)
    return jax.shard_map(
        functools.partial(on_device, sizes),
        mesh=mesh,
        in_specs=(spec, spec, spec),
        out_specs=(spec, spec),
        check_vma=False,
    )
```
